32 devices in a mesh: gx: 4 (over x, core), gy: 4 (over z), gz: 2 (over y).
Axes of the slice: x: 2, y: 2, z: 4, core: 2. Of those that a mesh axis runs over, the one named last changes fastest.
Arguments:
- columns: int32 [1024, 2048], P(('gx', 'gy', 'gz')), may hold values from 0 to 32767, as said below
- counts: int32 [1024, 2048], P(('gx', 'gy', 'gz')), may hold values from 1 to 63
- nnz_count: int32 [1024], P(('gx', 'gy', 'gz')), may hold values from 1 to 2048, as said below
- selected: int32 [2048], replicated, may hold values from 0 to 32767, as said below
Outputs:
- gene_stats: float32 [2, 32768], P(None, 'gz')
- pca_input: bfloat16 [1024, 2048], P(('gx', 'gy'), 'gz')
The draws below stay inside these ranges and needn't reach their ends.
Inputs may be any that keep to these rules, and one draw needn't show every extreme that they name: `columns`: in each row no two slots fall in the same block of 16 consecutive genes (so the first nnz_count slots hold distinct genes); slots beyond nnz_count are not part of the matrix. For every k, the live slots of one cell fall on at most 128 of the genes selected[k * 2048 / 2] to selected[(k + 1) * 2048 / 2 - 1]; some cell reaches 128 for every k in every draw. `nnz_count`: some cell has all 2048 slots live in every draw. `selected`: distinct genes.
All inputs are finite; a program needn't handle non-finite values.
Results may differ from the reference program's by a relative error of at most 0.0085.
Values may be sent and summed in bfloat16 or wider, within the bound.
No kernel may reach another device: no remote copies, remote signals or barrier semaphores. Data moves between devices by JAX's collectives and lax.ppermute only.
A program may use at most 128 MiB of HBM per device.

```python
import jax
import jax.numpy as jnp
from jax import lax

GENES = 32768
SEL = 2048
NNZ_MAX = 2048
CELLS = 1024
N_GZ = 2


def block_plan(key):
    stride = GENES // NNZ_MAX
    share_size = SEL // N_GZ
    per_owner = 2 * share_size // stride
    block_order = jax.random.permutation(jax.random.fold_in(key, 31), jnp.arange(NNZ_MAX, dtype=jnp.int32))[:N_GZ * per_owner]
    block_order = block_order.reshape(N_GZ, per_owner).astype(jnp.int32)
    block_keys = jax.random.split(jax.random.fold_in(key, 32), N_GZ * per_owner)
    lane_perm = jax.vmap(lambda one_key: jax.random.permutation(one_key, jnp.arange(stride, dtype=jnp.int32)))(block_keys)
    return (block_order, lane_perm.reshape(N_GZ, per_owner, stride).astype(jnp.int32))


def full_cell(key):
    return jax.random.randint(jax.random.fold_in(key, 41), (), 0, CELLS, dtype=jnp.int32)


def draw_columns(key, part):
    stride = GENES // NNZ_MAX
    block_order, lane_perm = block_plan(key)
    forced = jnp.full((NNZ_MAX,), -1, jnp.int32).at[block_order.reshape(-1)].set(lane_perm[:, :, 0].reshape(-1))
    jitter = jax.random.randint(jax.random.fold_in(key, 12), (CELLS, NNZ_MAX), 0, stride, dtype=jnp.int32)
    cell_ids = lax.broadcasted_iota(jnp.int32, (CELLS, NNZ_MAX), 0)
    pinned = (cell_ids == full_cell(key)) & (forced[None, :] >= 0)
    jitter = jnp.where(pinned, forced[None, :], jitter)
    block_ids = lax.broadcasted_iota(jnp.int32, (CELLS, NNZ_MAX), 1)
    genes_drawn = block_ids * stride + jitter
    shuffled = jax.random.permutation(jax.random.fold_in(key, 14), genes_drawn, axis=1, independent=True)
    return shuffled.astype(jnp.int32)


def draw_nnz_count(key, part):
    cell_ids = jnp.arange(CELLS, dtype=jnp.int32)
    lowest = NNZ_MAX // 3
    base = lowest + (NNZ_MAX - lowest) * cell_ids // max(CELLS - 1, 1)
    floor_count = jnp.maximum(base // 2, 1)
    spread = base - floor_count + 1
    draw_bits = jax.random.randint(jax.random.fold_in(key, 21), (CELLS,), 0, 1 << 20, dtype=jnp.int32)
    picked = floor_count + draw_bits * spread // (1 << 20)
    picked = jnp.where(cell_ids == full_cell(key), NNZ_MAX, picked)
    return jnp.clip(picked, 1, NNZ_MAX).astype(jnp.int32)


def draw_selected(key, part):
    stride = GENES // NNZ_MAX
    share_size = SEL // N_GZ
    per_owner = 2 * share_size // stride
    block_order, lane_perm = block_plan(key)
    gene_grid = block_order[:, :, None] * stride + lane_perm
    anchors = gene_grid[:, :, 0]
    others = gene_grid[:, :, 1:].reshape(N_GZ, per_owner * (stride - 1))
    other_keys = jax.random.split(jax.random.fold_in(key, 33), N_GZ)
    others = jax.vmap(lambda one_key, row_genes: jax.random.permutation(one_key, row_genes))(other_keys, others)
    others = others[:, :share_size - per_owner]
    chosen = jnp.concatenate([anchors, others], axis=1)
    order_keys = jax.random.split(jax.random.fold_in(key, 34), N_GZ)
    chosen = jax.vmap(lambda one_key, row_genes: jax.random.permutation(one_key, row_genes))(order_keys, chosen)
    return chosen.reshape(-1).astype(jnp.int32)


def with_ends(drawn, key, low, top_value):
    longest = drawn.shape.index(max(drawn.shape))
    spots = []
    for shift in (0, 1):
        where = [jax.random.randint(jax.random.fold_in(key, axis), (), 0, length) for axis, length in enumerate(drawn.shape)]
        where[longest] = (where[longest] + shift) % drawn.shape[longest]
        spots.append(tuple(where))
    return drawn.at[spots[0]].set(low).at[spots[1]].set(top_value)


def setup_inputs(seed: int = 0) -> dict:
    streams_of = jax.random.split(jax.random.key(seed), 5)
    return {
        "columns": draw_columns(jax.random.fold_in(streams_of[4], 71), 0),
        "counts": with_ends(jax.random.randint(streams_of[1], (CELLS, NNZ_MAX), 1, 64), jax.random.fold_in(streams_of[1], 1), 1, 63).astype(jnp.int32),
        "nnz_count": draw_nnz_count(jax.random.fold_in(streams_of[4], 71), 0),
        "selected": draw_selected(jax.random.fold_in(streams_of[4], 71), 0),
    }


target_sum = 10000.0
var_floor = 0.01
clip_value = 10.0

def reference(columns, counts, nnz_count, selected):
    slot = lax.broadcasted_iota(jnp.int32, counts.shape, 1)
    live = slot < nnz_count[:, None]
    raw = jnp.where(live, counts.astype(jnp.float32), jnp.float32(0.0))
    library = lax.optimization_barrier(jnp.sum(raw, axis=1, keepdims=True))
    values = jnp.log1p(raw * (target_sum / library))
    genes = jnp.where(live, columns, 0).astype(jnp.int32).reshape(-1)
    flat = values.reshape(-1)
    total = jax.ops.segment_sum(flat, genes, num_segments=GENES)
    square = jax.ops.segment_sum(flat * flat, genes, num_segments=GENES)
    mean = total / CELLS
    variance = square / CELLS - mean * mean
    gene_stats = jnp.stack([mean, variance])
    table = jnp.full((GENES,), SEL, jnp.int32).at[selected].set(jnp.arange(SEL, dtype=jnp.int32))
    position = table[genes]
    rows = jnp.repeat(jnp.arange(CELLS, dtype=jnp.int32), NNZ_MAX)
    index = rows * (SEL + 1) + position
    dense = jax.ops.segment_sum(flat, index, num_segments=CELLS * (SEL + 1)).reshape(CELLS, SEL + 1)[:, :SEL]
    mean_sel = mean[selected]
    scale_sel = jnp.sqrt(jnp.maximum(variance[selected], var_floor))
    pca_input = jnp.clip((dense - mean_sel[None, :]) / scale_sel[None, :], -clip_value, clip_value).astype(jnp.bfloat16)
    return (gene_stats, pca_input)
```

```python
import functools

import jax
import jax.numpy as jnp
from jax import lax
from jax.experimental import pallas as pl
from jax.experimental.pallas import tpu as pltpu
from jax.sharding import PartitionSpec as P

GENES = 32768
STRIDE = 16
LANES = 128
HIGH = GENES // (STRIDE * LANES)

target_sum = 10000.0
var_floor = 0.01
clip_value = 10.0

f32 = jnp.float32
bf16 = jnp.bfloat16


def tile_of_rows(ref, row, start, width):
    return jnp.broadcast_to(ref[pl.ds(row, 1), pl.ds(start, width)], (16, width)).astype(bf16)


def one_hot_lanes(low16, ids, width):
    groups = []
    for g in range(LANES // 16):
        hit = low16 == (ids + bf16(16.0 * g))
        groups.append(jnp.where(hit, bf16(1.0), bf16(0.0)))
    return groups


def scatter_kernel(owner_ref, columns_ref, counts_ref, nnz_ref, *refs, owners):
    compact_ref, scale_ref = refs[0], refs[1]
    total_refs = refs[2:2 + owners]
    low_s, high_s, off_s, count_s, total_s = refs[2 + owners:]
    rows, slots = columns_ref.shape
    i0 = lax.broadcasted_iota(jnp.int32, (rows, rows), 0)
    i1 = lax.broadcasted_iota(jnp.int32, (rows, rows), 1)
    nnz = jnp.broadcast_to(nnz_ref[...].astype(f32), (rows, rows))
    nnz = jnp.sum(jnp.where(i0 == i1, nnz, f32(0.0)), axis=1, keepdims=True).astype(jnp.int32)
    live = lax.broadcasted_iota(jnp.int32, (rows, slots), 1) < nnz
    columns = columns_ref[...]
    count = jnp.where(live, counts_ref[...], 0).astype(f32)
    count_s[...] = count
    low_s[...] = ((columns // STRIDE) % LANES).astype(f32)
    high_s[...] = jnp.where(live, columns // (STRIDE * LANES), -1).astype(f32)
    off_s[...] = (columns % STRIDE).astype(f32)
    library = jnp.sum(count, axis=1, keepdims=True)
    scale_ref[...] = jnp.broadcast_to(target_sum / library, (rows, LANES))
    width = min(256, slots)
    ids = lax.broadcasted_iota(jnp.int32, (16, width), 0).astype(f32).astype(bf16)

    def one_cell(c):
        acc = jnp.zeros((2 * HIGH, LANES), f32)
        for start in range(0, slots, width):
            low16 = tile_of_rows(low_s, c, start, width)
            high16 = tile_of_rows(high_s, c, start, width)
            off16 = tile_of_rows(off_s, c, start, width)
            count16 = tile_of_rows(count_s, c, start, width)
            table = jnp.concatenate(one_hot_lanes(low16, ids, width), axis=0)
            hit = high16 == ids
            payload = jnp.concatenate(
                [jnp.where(hit, off16, bf16(0.0)), jnp.where(hit, count16, bf16(0.0))], axis=0
            )
            acc = acc + lax.dot_general(
                payload, table, (((1,), (1,)), ((), ())), preferred_element_type=f32
            )
        base = pl.multiple_of(c * 2 * HIGH, 2 * HIGH)
        compact_ref[pl.ds(base, HIGH), :] = acc[:HIGH]
        compact_ref[pl.ds(base + HIGH, HIGH), :] = jnp.log(
            f32(1.0) + acc[HIGH:] * scale_ref[pl.ds(c, 1), :]
        )

    def cells(step, carry):
        for u in range(4):
            one_cell(step * 4 + u)
        return carry

    lax.fori_loop(0, rows // 4, cells, 0)

    def offsets(o, carry):
        o_f = o.astype(f32)
        total = jnp.zeros((HIGH, LANES), f32)
        square = jnp.zeros((HIGH, LANES), f32)
        for c in range(rows):
            off = compact_ref[pl.ds(c * 2 * HIGH, HIGH), :]
            value = compact_ref[pl.ds(c * 2 * HIGH + HIGH, HIGH), :]
            value = jnp.where(off == o_f, value, f32(0.0))
            total = total + value
            square = square + value * value
        total_s[0] = total
        total_s[1] = square
        own_high = HIGH // owners
        for d in range(owners):
            start = lax.rem(owner_ref[0] + d, owners) * own_high
            for s in range(2):
                total_refs[d][pl.ds((o * 2 + s) * own_high, own_high), :] = total_s[
                    s, pl.ds(start, own_high), :
                ]
        return carry

    lax.fori_loop(0, STRIDE, offsets, 0)


def select_kernel(owner_ref, compact_ref, scale_ref, selected_ref, *refs, owners):
    dense_refs = refs[:owners]
    sum_refs = refs[owners:2 * owners]
    pairs_s = refs[2 * owners]
    rows = scale_ref.shape[0]
    share = selected_ref.shape[1]
    width = min(256, share)
    for h in range(HIGH):
        lanes = pl.ds((h % 2) * LANES, LANES)
        pairs_s[h // 2, pl.ds(0, rows), lanes] = compact_ref[
            pl.ds(h, rows, stride=2 * HIGH), :
        ].astype(bf16)
        value = compact_ref[pl.ds(HIGH + h, rows, stride=2 * HIGH), :]
        upper = value.astype(bf16)
        pairs_s[h // 2, pl.ds(rows, rows), lanes] = upper
        pairs_s[h // 2, pl.ds(2 * rows, rows), lanes] = (value - upper.astype(f32)).astype(bf16)
    ids = lax.broadcasted_iota(jnp.int32, (16, width), 0).astype(f32).astype(bf16)
    for d in range(owners):
        owner = lax.rem(owner_ref[0] + d, owners)
        for start in range(0, share, width):
            picked = selected_ref[pl.ds(owner, 1), pl.ds(start, width)]
            low16 = jnp.broadcast_to(
                ((picked // STRIDE) % LANES).astype(f32), (16, width)
            ).astype(bf16)
            high16 = jnp.broadcast_to(
                (picked // (STRIDE * LANES)).astype(f32), (16, width)
            ).astype(bf16)
            low_hot = one_hot_lanes(low16, ids, width)
            acc = jnp.zeros((3 * rows, width), f32)
            for pair in range(HIGH // 2):
                parts = []
                for h in (2 * pair, 2 * pair + 1):
                    hit = high16 == bf16(float(h))
                    parts += [jnp.where(hit, part, bf16(0.0)) for part in low_hot]
                acc = acc + jnp.dot(
                    pairs_s[pair], jnp.concatenate(parts, axis=0), preferred_element_type=f32
                )
            off = (picked % STRIDE).astype(f32)
            value = acc[rows:2 * rows] + acc[2 * rows:]
            dense = jnp.where(acc[:rows] == off, value, f32(0.0))
            dense_refs[d][:, pl.ds(start, width)] = dense.astype(dense_refs[d].dtype)
            sum_refs[d][pl.ds(0, 1), pl.ds(start, width)] = jnp.sum(dense, axis=0, keepdims=True)
            sum_refs[d][pl.ds(1, 1), pl.ds(start, width)] = jnp.sum(
                dense * dense, axis=0, keepdims=True
            )


def shift(value, axis, d):
    n = lax.axis_size(axis)
    return lax.ppermute(value, axis, [(s, (s + d) % n) for s in range(n)])


def per_device(columns, counts, nnz_count, selected):
    rows, slots = columns.shape
    sel = selected.shape[0]
    owners = lax.axis_size("gz")
    outer = lax.axis_size("gx")
    middle = lax.axis_size("gy")
    cells = rows * outer * middle * owners
    owner = lax.axis_index("gz")
    place = lax.axis_index("gx")
    share = sel // owners
    own_high = HIGH // owners
    sum_rows = STRIDE * 2 * own_high
    vmem = pl.BlockSpec(memory_space=pltpu.VMEM)
    smem = pl.BlockSpec(memory_space=pltpu.SMEM)
    owner_arg = owner.reshape(1).astype(jnp.int32)

    made = pl.pallas_call(
        functools.partial(scatter_kernel, owners=owners),
        out_shape=[
            jax.ShapeDtypeStruct((rows * 2 * HIGH, LANES), f32),
            jax.ShapeDtypeStruct((rows, LANES), f32),
        ] + [jax.ShapeDtypeStruct((sum_rows, LANES), f32)] * owners,
        in_specs=[smem, vmem, vmem, vmem],
        out_specs=[vmem] * (2 + owners),
        scratch_shapes=[pltpu.VMEM((rows, slots), f32)] * 4 + [pltpu.VMEM((2, HIGH, LANES), f32)],
        name="scatter",
    )(owner_arg, columns, counts, nnz_count.reshape(1, rows))
    compact, scale, sums = made[0], made[1], made[2:]
    moved_sums = [shift(sums[d], "gz", d) for d in range(1, owners)]

    picked = pl.pallas_call(
        functools.partial(select_kernel, owners=owners),
        out_shape=[jax.ShapeDtypeStruct((rows, share), f32)]
        + [jax.ShapeDtypeStruct((rows, share), bf16)] * (owners - 1)
        + [jax.ShapeDtypeStruct((2, share), f32)] * owners,
        in_specs=[smem, vmem, vmem, vmem],
        out_specs=[vmem] * (2 * owners),
        scratch_shapes=[pltpu.VMEM((HIGH // 2, 3 * rows, 2 * LANES), bf16)],
        name="select",
    )(owner_arg, compact, scale, selected.reshape(owners, share))
    dense, picked_sums = picked[:owners], picked[owners:]
    moved_picked = [shift(picked_sums[d], "gz", d) for d in range(1, owners)]
    moved_dense = [shift(dense[d], "gz", d) for d in range(1, owners)]

    gene_sums = functools.reduce(jnp.add, [sums[0]] + moved_sums)
    sel_sums = functools.reduce(jnp.add, [picked_sums[0]] + moved_picked)
    chunk_rows = sum_rows // outer
    sel_part = sel_sums.reshape(2, outer, share // outer).transpose(1, 0, 2).reshape(outer, -1)
    extra = -(-sel_part.shape[1] // (8 * LANES)) * 8
    sel_part = jnp.pad(sel_part, ((0, 0), (0, extra * LANES - sel_part.shape[1])))
    both = jnp.concatenate(
        [gene_sums.reshape(outer, chunk_rows, LANES), sel_part.reshape(outer, extra, LANES)], axis=1
    )

    def chunk(index):
        return lax.dynamic_index_in_dim(both, index, 0, keepdims=False)

    part = functools.reduce(
        jnp.add,
        [chunk(place)] + [shift(chunk(lax.rem(place + d, outer)), "gx", d) for d in range(1, outer)],
    )
    part = functools.reduce(jnp.add, [part] + [shift(part, "gy", d) for d in range(1, middle)])
    held = jnp.stack([part] + [shift(part, "gx", d) for d in range(1, outer)])
    full = jnp.stack(
        [
            lax.dynamic_index_in_dim(held, lax.rem(place + outer - i, outer), 0, keepdims=False)
            for i in range(outer)
        ]
    )
    genes = full[:, :chunk_rows].reshape(STRIDE, 2, own_high * LANES)
    mean = genes[:, 0] / cells
    variance = genes[:, 1] / cells - mean * mean
    gene_stats = jnp.stack([mean, variance]).transpose(0, 2, 1).reshape(2, -1)
    part_size = share // outer
    sel_full = full[:, chunk_rows:].reshape(outer, -1)[:, :2 * part_size]
    sel_full = sel_full.reshape(outer, 2, part_size).transpose(1, 0, 2).reshape(2, share)
    sel_mean = sel_full[0] / cells
    sel_variance = sel_full[1] / cells - sel_mean * sel_mean
    sel_scale = jnp.sqrt(jnp.maximum(sel_variance, var_floor))
    blocks = jnp.stack([dense[0]] + [m.astype(f32) for m in moved_dense])
    ordered = jnp.concatenate(
        [
            lax.dynamic_index_in_dim(blocks, lax.rem(owner + owners - q, owners), 0, keepdims=False)
            for q in range(owners)
        ],
        axis=0,
    )
    pca_input = jnp.clip((ordered - sel_mean) / sel_scale, -clip_value, clip_value).astype(bf16)
    return (gene_stats, pca_input)


def solution(mesh):
    return jax.shard_map(
        per_device,
        mesh=mesh,
        in_specs=(
            P(("gx", "gy", "gz"), None),
            P(("gx", "gy", "gz"), None),
            P(("gx", "gy", "gz")),
            P(),
        ),
        out_specs=(P(None, "gz"), P(("gx", "gy"), "gz")),
        check_vma=False,
    )
```

```python
import functools

import jax
import jax.numpy as jnp
from jax import lax
from jax.experimental import pallas as pl
from jax.experimental.pallas import tpu as pltpu
from jax.sharding import PartitionSpec as P

GENES = 32768
STRIDE = 16
LANES = 128
HIGH = GENES // (STRIDE * LANES)
HALF = LANES // 2
STRIDE_BITS = STRIDE.bit_length() - 1
ROW_BITS = (STRIDE * LANES).bit_length() - 1
HALF_BITS = (STRIDE * HALF).bit_length() - 1

target_sum = 10000.0
var_floor = 0.01
clip_value = 10.0

f32 = jnp.float32
bf16 = jnp.bfloat16


def tile_of_rows(ref, row, start, width):
    return jnp.broadcast_to(ref[pl.ds(row, 1), pl.ds(start, width)], (16, width)).astype(bf16)


def one_hot_lanes(low16, ids, lanes):
    groups = []
    for g in range(lanes // 16):
        hit = low16 == (ids + bf16(16.0 * g))
        groups.append(jnp.where(hit, bf16(1.0), bf16(0.0)))
    return groups


def scatter_kernel(owner_ref, columns_ref, counts_ref, nnz_ref, *refs, owners):
    compact_ref, scale_ref = refs[0], refs[1]
    total_refs = refs[2:2 + owners]
    low_s, high_s, off_s, count_s, total_s = refs[2 + owners:]
    rows, slots = columns_ref.shape
    i0 = lax.broadcasted_iota(jnp.int32, (rows, rows), 0)
    i1 = lax.broadcasted_iota(jnp.int32, (rows, rows), 1)
    nnz = jnp.broadcast_to(nnz_ref[...].astype(f32), (rows, rows))
    nnz = jnp.sum(jnp.where(i0 == i1, nnz, f32(0.0)), axis=1, keepdims=True).astype(jnp.int32)
    live = lax.broadcasted_iota(jnp.int32, (rows, slots), 1) < nnz
    columns = columns_ref[...]
    count = jnp.where(live, counts_ref[...], 0).astype(f32)
    count_s[...] = count
    low_s[...] = ((columns >> STRIDE_BITS) & (HALF - 1)).astype(f32)
    row = (columns >> ROW_BITS) + ((columns >> HALF_BITS) & 1) * HIGH
    high_s[...] = jnp.where(live, row, -1).astype(f32)
    off_s[...] = (columns & (STRIDE - 1)).astype(f32)
    library = jnp.sum(count, axis=1, keepdims=True)
    scale_ref[...] = jnp.broadcast_to(target_sum / library, (rows, LANES))
    width = min(256, slots)
    ids = lax.broadcasted_iota(jnp.int32, (16, width), 0).astype(f32).astype(bf16)

    def one_cell(c):
        acc = jnp.zeros((4 * HIGH, HALF), f32)
        for start in range(0, slots, width):
            low16 = tile_of_rows(low_s, c, start, width)
            high16 = tile_of_rows(high_s, c, start, width)
            off16 = tile_of_rows(off_s, c, start, width)
            count16 = tile_of_rows(count_s, c, start, width)
            table = jnp.concatenate(one_hot_lanes(low16, ids, HALF), axis=0)
            hits = [high16 == ids, high16 == ids + bf16(float(HIGH))]
            payload = jnp.concatenate(
                [jnp.where(hit, part, bf16(0.0)) for part in (off16, count16) for hit in hits],
                axis=0,
            )
            acc = acc + lax.dot_general(
                payload, table, (((1,), (1,)), ((), ())), preferred_element_type=f32
            )
        base = pl.multiple_of(c * 2 * HIGH, 2 * HIGH)
        off = jnp.concatenate([acc[:HIGH], acc[HIGH:2 * HIGH]], axis=1)
        count = jnp.concatenate([acc[2 * HIGH:3 * HIGH], acc[3 * HIGH:]], axis=1)
        compact_ref[pl.ds(base, HIGH), :] = off
        compact_ref[pl.ds(base + HIGH, HIGH), :] = jnp.log(
            f32(1.0) + count * scale_ref[pl.ds(c, 1), :]
        )

    def cells(step, carry):
        for u in range(4):
            one_cell(step * 4 + u)
        return carry

    lax.fori_loop(0, rows // 4, cells, 0)

    own_high = HIGH // owners
    together = 4

    def offsets(step, carry):
        first = step * together
        totals = [jnp.zeros((HIGH, LANES), f32)] * together
        squares = [jnp.zeros((HIGH, LANES), f32)] * together
        for c in range(rows):
            off = compact_ref[pl.ds(c * 2 * HIGH, HIGH), :]
            value = compact_ref[pl.ds(c * 2 * HIGH + HIGH, HIGH), :]
            for u in range(together):
                mine = jnp.where(off == (first + u).astype(f32), value, f32(0.0))
                totals[u] = totals[u] + mine
                squares[u] = squares[u] + mine * mine
        for u in range(together):
            total_s[0] = totals[u]
            total_s[1] = squares[u]
            for d in range(owners):
                start = lax.rem(owner_ref[0] + d, owners) * own_high
                for s in range(2):
                    target = ((first + u) * 2 + s) * own_high
                    total_refs[d][pl.ds(target, own_high), :] = total_s[s, pl.ds(start, own_high), :]
        return carry

    lax.fori_loop(0, STRIDE // together, offsets, 0)


def select_kernel(owner_ref, compact_ref, scale_ref, selected_ref, *refs, owners):
    dense_refs = refs[:owners]
    sum_refs = refs[owners:2 * owners]
    pairs_s = refs[2 * owners]
    rows = scale_ref.shape[0]
    share = selected_ref.shape[1] // owners
    share_rows = share // LANES
    width = min(256, share)
    for h in range(HIGH):
        lanes = pl.ds((h % 2) * LANES, LANES)
        pairs_s[h // 2, pl.ds(0, rows), lanes] = compact_ref[
            pl.ds(h, rows, stride=2 * HIGH), :
        ].astype(bf16)
        value = compact_ref[pl.ds(HIGH + h, rows, stride=2 * HIGH), :]
        upper = value.astype(bf16)
        pairs_s[h // 2, pl.ds(rows, rows), lanes] = upper
        pairs_s[h // 2, pl.ds(2 * rows, rows), lanes] = (value - upper.astype(f32)).astype(bf16)
    ids = lax.broadcasted_iota(jnp.int32, (16, width), 0).astype(f32).astype(bf16)
    for d in range(owners):
        owner = lax.rem(owner_ref[0] + d, owners)
        for start in range(0, share, width):
            place = pl.multiple_of(owner * share + start, LANES)
            picked = selected_ref[:, pl.ds(place, width)]
            low16 = jnp.broadcast_to(
                ((picked >> STRIDE_BITS) & (LANES - 1)).astype(f32), (16, width)
            ).astype(bf16)
            high16 = jnp.broadcast_to(
                (picked >> ROW_BITS).astype(f32), (16, width)
            ).astype(bf16)
            low_hot = one_hot_lanes(low16, ids, LANES)
            acc = jnp.zeros((3 * rows, width), f32)
            for pair in range(HIGH // 2):
                parts = []
                for h in (2 * pair, 2 * pair + 1):
                    hit = high16 == bf16(float(h))
                    parts += [jnp.where(hit, part, bf16(0.0)) for part in low_hot]
                acc = acc + jnp.dot(
                    pairs_s[pair], jnp.concatenate(parts, axis=0), preferred_element_type=f32
                )
            off = (picked & (STRIDE - 1)).astype(f32)
            value = acc[rows:2 * rows] + acc[2 * rows:]
            dense = jnp.where(acc[:rows] == off, value, f32(0.0))
            dense_refs[d][:, pl.ds(start, width)] = dense.astype(dense_refs[d].dtype)
            stats = [
                jnp.sum(dense, axis=0, keepdims=True),
                jnp.sum(dense * dense, axis=0, keepdims=True),
            ]
            for s in range(2):
                for q in range(width // LANES):
                    target = s * share_rows + start // LANES + q
                    sum_refs[d][pl.ds(target, 1), :] = stats[s][:, q * LANES:(q + 1) * LANES]


def shift(value, axis, d):
    n = lax.axis_size(axis)
    return lax.ppermute(value, axis, [(s, (s + d) % n) for s in range(n)])


def paired(n):
    return n & (n - 1) == 0


def exchange(value, axis, d):
    n = lax.axis_size(axis)
    if not paired(n):
        return shift(value, axis, d)
    return lax.ppermute(value, axis, [(s, s ^ d) for s in range(n)])


def tree_sum(terms):
    while len(terms) > 1:
        last = terms[len(terms) - len(terms) % 2:]
        terms = [terms[i] + terms[i + 1] for i in range(0, len(terms) - 1, 2)] + last
    return terms[0]


def target_of(place, d, n):
    return place ^ d if paired(n) else lax.rem(place + d, n)


def slot_of(place, i, n):
    return place ^ i if paired(n) else lax.rem(place + n - i, n)


def per_device(columns, counts, nnz_count, selected):
    rows, slots = columns.shape
    sel = selected.shape[0]
    owners = lax.axis_size("gz")
    outer = lax.axis_size("gx")
    middle = lax.axis_size("gy")
    cells = rows * outer * middle * owners
    owner = lax.axis_index("gz")
    place = lax.axis_index("gx")
    share = sel // owners
    own_high = HIGH // owners
    sum_rows = STRIDE * 2 * own_high
    vmem = pl.BlockSpec(memory_space=pltpu.VMEM)
    smem = pl.BlockSpec(memory_space=pltpu.SMEM)
    owner_arg = owner.reshape(1).astype(jnp.int32)

    made = pl.pallas_call(
        functools.partial(scatter_kernel, owners=owners),
        out_shape=[
            jax.ShapeDtypeStruct((rows * 2 * HIGH, LANES), f32),
            jax.ShapeDtypeStruct((rows, LANES), f32),
        ] + [jax.ShapeDtypeStruct((sum_rows, LANES), f32)] * owners,
        in_specs=[smem, vmem, vmem, vmem],
        out_specs=[vmem] * (2 + owners),
        scratch_shapes=[pltpu.VMEM((rows, slots), f32)] * 4 + [pltpu.VMEM((2, HIGH, LANES), f32)],
        name="scatter",
    )(owner_arg, columns, counts, nnz_count.reshape(1, rows))
    compact, scale, sums = made[0], made[1], made[2:]
    moved_sums = [shift(sums[d], "gz", d) for d in range(1, owners)]

    picked = pl.pallas_call(
        functools.partial(select_kernel, owners=owners),
        out_shape=[jax.ShapeDtypeStruct((rows, share), f32)]
        + [jax.ShapeDtypeStruct((rows, share), bf16)] * (owners - 1)
        + [jax.ShapeDtypeStruct((2 * share // LANES, LANES), f32)] * owners,
        in_specs=[smem, vmem, vmem, vmem],
        out_specs=[vmem] * (2 * owners),
        scratch_shapes=[pltpu.VMEM((HIGH // 2, 3 * rows, 2 * LANES), bf16)],
        name="select",
    )(owner_arg, compact, scale, selected.reshape(1, sel))
    dense, picked_sums = picked[:owners], picked[owners:]
    moved_picked = [shift(picked_sums[d], "gz", d) for d in range(1, owners)]
    moved_dense = [shift(dense[d], "gz", d) for d in range(1, owners)]

    gene_sums = functools.reduce(jnp.add, [sums[0]] + moved_sums)
    sel_sums = functools.reduce(jnp.add, [picked_sums[0]] + moved_picked)
    chunk_rows = sum_rows // outer
    chunks = gene_sums.reshape(outer, chunk_rows, LANES)

    def chunk(d):
        return lax.dynamic_index_in_dim(chunks, target_of(place, d, outer), 0, keepdims=False)

    part = functools.reduce(
        jnp.add, [chunk(0)] + [exchange(chunk(d), "gx", d) for d in range(1, outer)]
    )
    part = jnp.concatenate([part, sel_sums], axis=0)
    part = tree_sum([part] + [exchange(part, "gy", d) for d in range(1, middle)])
    held = jnp.stack([part] + [exchange(part, "gx", d) for d in range(1, outer)])
    full = jnp.stack(
        [
            lax.dynamic_index_in_dim(held[:, :chunk_rows], slot_of(place, i, outer), 0, keepdims=False)
            for i in range(outer)
        ]
    )
    genes = full.reshape(STRIDE, 2, own_high * LANES)
    mean = genes[:, 0] / cells
    variance = genes[:, 1] / cells - mean * mean
    gene_stats = jnp.stack([mean, variance]).transpose(0, 2, 1).reshape(2, -1)
    sel_full = jnp.sum(held[:, chunk_rows:], axis=0).reshape(2, share)
    sel_mean = sel_full[0] / cells
    sel_variance = sel_full[1] / cells - sel_mean * sel_mean
    sel_scale = jnp.sqrt(jnp.maximum(sel_variance, var_floor))
    blocks = jnp.stack([dense[0]] + [m.astype(f32) for m in moved_dense])
    ordered = jnp.concatenate(
        [
            lax.dynamic_index_in_dim(blocks, lax.rem(owner + owners - q, owners), 0, keepdims=False)
            for q in range(owners)
        ],
        axis=0,
    )
    pca_input = jnp.clip((ordered - sel_mean) / sel_scale, -clip_value, clip_value).astype(bf16)
    return (gene_stats, pca_input)


def solution(mesh):
    return jax.shard_map(
        per_device,
        mesh=mesh,
        in_specs=(
            P(("gx", "gy", "gz"), None),
            P(("gx", "gy", "gz"), None),
            P(("gx", "gy", "gz")),
            P(),
        ),
        out_specs=(P(None, "gz"), P(("gx", "gy"), "gz")),
        check_vma=False,
    )
```

```python
import functools

import jax
import jax.numpy as jnp
from jax import lax
from jax.experimental import pallas as pl
from jax.experimental.pallas import tpu as pltpu
from jax.sharding import PartitionSpec as P

GENES = 32768
STRIDE = 16
LANES = 128
HIGH = GENES // (STRIDE * LANES)
HALF = LANES // 2
STRIDE_BITS = STRIDE.bit_length() - 1
ROW_BITS = (STRIDE * LANES).bit_length() - 1
HALF_BITS = (STRIDE * HALF).bit_length() - 1

target_sum = 10000.0
var_floor = 0.01
clip_value = 10.0

f32 = jnp.float32
bf16 = jnp.bfloat16


def tile_of_rows(ref, row, start, width):
    return jnp.broadcast_to(ref[pl.ds(row, 1), pl.ds(start, width)], (16, width)).astype(bf16)


def one_hot_lanes(low16, ids, lanes):
    groups = []
    for g in range(lanes // 16):
        hit = low16 == (ids + bf16(16.0 * g))
        groups.append(jnp.where(hit, bf16(1.0), bf16(0.0)))
    return groups


def scatter_kernel(owner_ref, columns_ref, counts_ref, nnz_ref, *refs, owners):
    compact_ref, scale_ref = refs[0], refs[1]
    total_refs = refs[2:2 + owners]
    low_s, high_s, off_s, count_s, total_s = refs[2 + owners:]
    rows, slots = columns_ref.shape
    i0 = lax.broadcasted_iota(jnp.int32, (rows, rows), 0)
    i1 = lax.broadcasted_iota(jnp.int32, (rows, rows), 1)
    nnz = jnp.broadcast_to(nnz_ref[...].astype(f32), (rows, rows))
    nnz = jnp.sum(jnp.where(i0 == i1, nnz, f32(0.0)), axis=1, keepdims=True).astype(jnp.int32)
    live = lax.broadcasted_iota(jnp.int32, (rows, slots), 1) < nnz
    columns = columns_ref[...]
    count = jnp.where(live, counts_ref[...], 0).astype(f32)
    count_s[...] = count
    low_s[...] = ((columns >> STRIDE_BITS) & (HALF - 1)).astype(f32)
    row = (columns >> ROW_BITS) + ((columns >> HALF_BITS) & 1) * HIGH
    high_s[...] = jnp.where(live, row, -1).astype(f32)
    off_s[...] = (columns & (STRIDE - 1)).astype(f32)
    library = jnp.sum(count, axis=1, keepdims=True)
    scale_ref[...] = jnp.broadcast_to(target_sum / library, (rows, LANES))
    width = min(256, slots)
    ids = lax.broadcasted_iota(jnp.int32, (16, width), 0).astype(f32).astype(bf16)

    def one_cell(c):
        acc = jnp.zeros((4 * HIGH, HALF), f32)
        for start in range(0, slots, width):
            low16 = tile_of_rows(low_s, c, start, width)
            high16 = tile_of_rows(high_s, c, start, width)
            off16 = tile_of_rows(off_s, c, start, width)
            count16 = tile_of_rows(count_s, c, start, width)
            table = jnp.concatenate(one_hot_lanes(low16, ids, HALF), axis=0)
            hits = [high16 == ids, high16 == ids + bf16(float(HIGH))]
            payload = jnp.concatenate(
                [jnp.where(hit, part, bf16(0.0)) for part in (off16, count16) for hit in hits],
                axis=0,
            )
            acc = acc + lax.dot_general(
                payload, table, (((1,), (1,)), ((), ())), preferred_element_type=f32
            )
        base = pl.multiple_of(c * 2 * HIGH, 2 * HIGH)
        off = jnp.concatenate([acc[:HIGH], acc[HIGH:2 * HIGH]], axis=1)
        count = jnp.concatenate([acc[2 * HIGH:3 * HIGH], acc[3 * HIGH:]], axis=1)
        compact_ref[pl.ds(base, HIGH), :] = off
        compact_ref[pl.ds(base + HIGH, HIGH), :] = jnp.log(
            f32(1.0) + count * scale_ref[pl.ds(c, 1), :]
        )

    def cells(step, carry):
        for u in range(4):
            one_cell(step * 4 + u)
        return carry

    lax.fori_loop(0, rows // 4, cells, 0)

    own_high = HIGH // owners
    together = 4

    def offsets(step, carry):
        first = step * together
        totals = [jnp.zeros((HIGH, LANES), f32)] * together
        squares = [jnp.zeros((HIGH, LANES), f32)] * together
        for c in range(rows):
            off = compact_ref[pl.ds(c * 2 * HIGH, HIGH), :]
            value = compact_ref[pl.ds(c * 2 * HIGH + HIGH, HIGH), :]
            for u in range(together):
                mine = jnp.where(off == (first + u).astype(f32), value, f32(0.0))
                totals[u] = totals[u] + mine
                squares[u] = squares[u] + mine * mine
        for u in range(together):
            total_s[0] = totals[u]
            total_s[1] = squares[u]
            for d in range(owners):
                start = lax.rem(owner_ref[0] + d, owners) * own_high
                for s in range(2):
                    target = ((first + u) * 2 + s) * own_high
                    total_refs[d][pl.ds(target, own_high), :] = total_s[s, pl.ds(start, own_high), :]
        return carry

    lax.fori_loop(0, STRIDE // together, offsets, 0)


def select_kernel(owner_ref, compact_ref, scale_ref, selected_ref, *refs, owners):
    dense_refs = refs[:owners]
    sum_refs = refs[owners:2 * owners]
    pairs_s = refs[2 * owners]
    rows = scale_ref.shape[0]
    share = selected_ref.shape[1] // owners
    share_rows = share // LANES
    width = min(256, share)
    for h in range(HIGH):
        lanes = pl.ds((h % 2) * LANES, LANES)
        pairs_s[h // 2, pl.ds(0, rows), lanes] = compact_ref[
            pl.ds(h, rows, stride=2 * HIGH), :
        ].astype(bf16)
        value = compact_ref[pl.ds(HIGH + h, rows, stride=2 * HIGH), :]
        upper = value.astype(bf16)
        pairs_s[h // 2, pl.ds(rows, rows), lanes] = upper
        pairs_s[h // 2, pl.ds(2 * rows, rows), lanes] = (value - upper.astype(f32)).astype(bf16)
    ids = lax.broadcasted_iota(jnp.int32, (16, width), 0).astype(f32).astype(bf16)
    for d in range(owners):
        owner = lax.rem(owner_ref[0] + d, owners)
        for start in range(0, share, width):
            place = pl.multiple_of(owner * share + start, LANES)
            picked = selected_ref[:, pl.ds(place, width)]
            low16 = jnp.broadcast_to(
                ((picked >> STRIDE_BITS) & (LANES - 1)).astype(f32), (16, width)
            ).astype(bf16)
            high16 = jnp.broadcast_to(
                (picked >> ROW_BITS).astype(f32), (16, width)
            ).astype(bf16)
            low_hot = one_hot_lanes(low16, ids, LANES)
            acc = jnp.zeros((3 * rows, width), f32)
            for pair in range(HIGH // 2):
                parts = []
                for h in (2 * pair, 2 * pair + 1):
                    hit = high16 == bf16(float(h))
                    parts += [jnp.where(hit, part, bf16(0.0)) for part in low_hot]
                acc = acc + jnp.dot(
                    pairs_s[pair], jnp.concatenate(parts, axis=0), preferred_element_type=f32
                )
            off = (picked & (STRIDE - 1)).astype(f32)
            value = acc[rows:2 * rows] + acc[2 * rows:]
            dense = jnp.where(acc[:rows] == off, value, f32(0.0))
            dense_refs[d][:, pl.ds(start, width)] = dense.astype(dense_refs[d].dtype)
            stats = [
                jnp.sum(dense, axis=0, keepdims=True),
                jnp.sum(dense * dense, axis=0, keepdims=True),
            ]
            for s in range(2):
                for q in range(width // LANES):
                    target = s * share_rows + start // LANES + q
                    sum_refs[d][pl.ds(target, 1), :] = stats[s][:, q * LANES:(q + 1) * LANES]


def shift(value, axis, d):
    n = lax.axis_size(axis)
    return lax.ppermute(value, axis, [(s, (s + d) % n) for s in range(n)])


def paired(n):
    return n & (n - 1) == 0


def exchange(value, axis, d):
    n = lax.axis_size(axis)
    if not paired(n):
        return shift(value, axis, d)
    return lax.ppermute(value, axis, [(s, s ^ d) for s in range(n)])


def tree_sum(terms):
    while len(terms) > 1:
        last = terms[len(terms) - len(terms) % 2:]
        terms = [terms[i] + terms[i + 1] for i in range(0, len(terms) - 1, 2)] + last
    return terms[0]


def target_of(place, d, n):
    return place ^ d if paired(n) else lax.rem(place + d, n)


def slot_of(place, i, n):
    return place ^ i if paired(n) else lax.rem(place + n - i, n)


def per_device(columns, counts, nnz_count, selected):
    rows, slots = columns.shape
    sel = selected.shape[0]
    owners = lax.axis_size("gz")
    outer = lax.axis_size("gx")
    middle = lax.axis_size("gy")
    cells = rows * outer * middle * owners
    owner = lax.axis_index("gz")
    place = lax.axis_index("gx")
    share = sel // owners
    own_high = HIGH // owners
    sum_rows = STRIDE * 2 * own_high
    vmem = pl.BlockSpec(memory_space=pltpu.VMEM)
    smem = pl.BlockSpec(memory_space=pltpu.SMEM)
    owner_arg = owner.reshape(1).astype(jnp.int32)

    made = pl.pallas_call(
        functools.partial(scatter_kernel, owners=owners),
        out_shape=[
            jax.ShapeDtypeStruct((rows * 2 * HIGH, LANES), f32),
            jax.ShapeDtypeStruct((rows, LANES), f32),
        ] + [jax.ShapeDtypeStruct((sum_rows, LANES), f32)] * owners,
        in_specs=[smem, vmem, vmem, vmem],
        out_specs=[vmem] * (2 + owners),
        scratch_shapes=[pltpu.VMEM((rows, slots), f32)] * 4 + [pltpu.VMEM((2, HIGH, LANES), f32)],
        name="scatter",
    )(owner_arg, columns, counts, nnz_count.reshape(1, rows))
    compact, scale, sums = made[0], made[1], made[2:]
    moved_sums = [shift(sums[d], "gz", d) for d in range(1, owners)]

    picked = pl.pallas_call(
        functools.partial(select_kernel, owners=owners),
        out_shape=[jax.ShapeDtypeStruct((rows, share), f32)]
        + [jax.ShapeDtypeStruct((rows, share), bf16)] * (owners - 1)
        + [jax.ShapeDtypeStruct((2 * share // LANES, LANES), f32)] * owners,
        in_specs=[smem, vmem, vmem, vmem],
        out_specs=[vmem] * (2 * owners),
        scratch_shapes=[pltpu.VMEM((HIGH // 2, 3 * rows, 2 * LANES), bf16)],
        name="select",
    )(owner_arg, compact, scale, selected.reshape(1, sel))
    own_sums, *picked = lax.optimization_barrier((sums[0], *picked))
    dense, picked_sums = picked[:owners], picked[owners:]
    moved_picked = [shift(picked_sums[d], "gz", d) for d in range(1, owners)]
    moved_dense = [shift(dense[d], "gz", d) for d in range(1, owners)]

    gene_sums = functools.reduce(jnp.add, [own_sums] + moved_sums)
    sel_sums = functools.reduce(jnp.add, [picked_sums[0]] + moved_picked)
    chunk_rows = sum_rows // outer
    chunks = gene_sums.reshape(outer, chunk_rows, LANES)

    def chunk(d):
        return lax.dynamic_index_in_dim(chunks, target_of(place, d, outer), 0, keepdims=False)

    part = functools.reduce(
        jnp.add, [chunk(0)] + [exchange(chunk(d), "gx", d) for d in range(1, outer)]
    )
    part = jnp.concatenate([part, sel_sums], axis=0)
    part = tree_sum([part] + [exchange(part, "gy", d) for d in range(1, middle)])
    held = jnp.stack([part] + [exchange(part, "gx", d) for d in range(1, outer)])
    full = jnp.stack(
        [
            lax.dynamic_index_in_dim(held[:, :chunk_rows], slot_of(place, i, outer), 0, keepdims=False)
            for i in range(outer)
        ]
    )
    genes = full.reshape(STRIDE, 2, own_high * LANES)
    mean = genes[:, 0] / cells
    variance = genes[:, 1] / cells - mean * mean
    gene_stats = jnp.stack([mean, variance]).transpose(0, 2, 1).reshape(2, -1)
    sel_full = jnp.sum(held[:, chunk_rows:], axis=0).reshape(2, share)
    sel_mean = sel_full[0] / cells
    sel_variance = sel_full[1] / cells - sel_mean * sel_mean
    sel_scale = jnp.sqrt(jnp.maximum(sel_variance, var_floor))
    blocks = jnp.stack([dense[0]] + [m.astype(f32) for m in moved_dense])
    ordered = jnp.concatenate(
        [
            lax.dynamic_index_in_dim(blocks, lax.rem(owner + owners - q, owners), 0, keepdims=False)
            for q in range(owners)
        ],
        axis=0,
    )
    pca_input = jnp.clip((ordered - sel_mean) / sel_scale, -clip_value, clip_value).astype(bf16)
    return (gene_stats, pca_input)


def solution(mesh):
    return jax.shard_map(
        per_device,
        mesh=mesh,
        in_specs=(
            P(("gx", "gy", "gz"), None),
            P(("gx", "gy", "gz"), None),
            P(("gx", "gy", "gz")),
            P(),
        ),
        out_specs=(P(None, "gz"), P(("gx", "gy"), "gz")),
        check_vma=False,
    )
```

```python
import functools

import jax
import jax.numpy as jnp
from jax import lax
from jax.experimental import pallas as pl
from jax.experimental.pallas import tpu as pltpu
from jax.sharding import PartitionSpec as P

GENES = 32768
STRIDE = 16
LANES = 128
HIGH = GENES // (STRIDE * LANES)
HALF = LANES // 2
STRIDE_BITS = STRIDE.bit_length() - 1
ROW_BITS = (STRIDE * LANES).bit_length() - 1
HALF_BITS = (STRIDE * HALF).bit_length() - 1

target_sum = 10000.0
var_floor = 0.01
clip_value = 10.0

f32 = jnp.float32
bf16 = jnp.bfloat16


def tile_of_rows(ref, row, start, width):
    return jnp.broadcast_to(ref[pl.ds(row, 1), pl.ds(start, width)], (16, width)).astype(bf16)


def one_hot_lanes(low16, ids, lanes):
    groups = []
    for g in range(lanes // 16):
        hit = low16 == (ids + bf16(16.0 * g))
        groups.append(jnp.where(hit, bf16(1.0), bf16(0.0)))
    return groups


def scatter_kernel(owner_ref, columns_ref, counts_ref, nnz_ref, *refs, owners):
    compact_ref, scale_ref = refs[0], refs[1]
    total_refs = refs[2:2 + owners]
    low_s, high_s, off_s, count_s, total_s = refs[2 + owners:]
    rows, slots = columns_ref.shape
    i0 = lax.broadcasted_iota(jnp.int32, (rows, rows), 0)
    i1 = lax.broadcasted_iota(jnp.int32, (rows, rows), 1)
    nnz = jnp.broadcast_to(nnz_ref[...].astype(f32), (rows, rows))
    nnz = jnp.sum(jnp.where(i0 == i1, nnz, f32(0.0)), axis=1, keepdims=True).astype(jnp.int32)
    live = lax.broadcasted_iota(jnp.int32, (rows, slots), 1) < nnz
    columns = columns_ref[...]
    count = jnp.where(live, counts_ref[...], 0).astype(f32)
    count_s[...] = count
    low_s[...] = ((columns >> STRIDE_BITS) & (HALF - 1)).astype(f32)
    row = (columns >> ROW_BITS) + ((columns >> HALF_BITS) & 1) * HIGH
    high_s[...] = jnp.where(live, row, -1).astype(f32)
    off_s[...] = (columns & (STRIDE - 1)).astype(f32)
    library = jnp.sum(count, axis=1, keepdims=True)
    scale_ref[...] = jnp.broadcast_to(target_sum / library, (rows, LANES))
    width = min(256, slots)
    ids = lax.broadcasted_iota(jnp.int32, (16, width), 0).astype(f32).astype(bf16)

    def one_cell(c):
        acc = jnp.zeros((4 * HIGH, HALF), f32)
        for start in range(0, slots, width):
            low16 = tile_of_rows(low_s, c, start, width)
            high16 = tile_of_rows(high_s, c, start, width)
            off16 = tile_of_rows(off_s, c, start, width)
            count16 = tile_of_rows(count_s, c, start, width)
            table = jnp.concatenate(one_hot_lanes(low16, ids, HALF), axis=0)
            hits = [high16 == ids, high16 == ids + bf16(float(HIGH))]
            payload = jnp.concatenate(
                [jnp.where(hit, part, bf16(0.0)) for part in (off16, count16) for hit in hits],
                axis=0,
            )
            acc = acc + lax.dot_general(
                payload, table, (((1,), (1,)), ((), ())), preferred_element_type=f32
            )
        base = pl.multiple_of(c * 2 * HIGH, 2 * HIGH)
        off = jnp.concatenate([acc[:HIGH], acc[HIGH:2 * HIGH]], axis=1)
        count = jnp.concatenate([acc[2 * HIGH:3 * HIGH], acc[3 * HIGH:]], axis=1)
        compact_ref[pl.ds(base, HIGH), :] = off
        compact_ref[pl.ds(base + HIGH, HIGH), :] = jnp.log(
            f32(1.0) + count * scale_ref[pl.ds(c, 1), :]
        )

    def cells(step, carry):
        for u in range(8):
            one_cell(step * 8 + u)
        return carry

    lax.fori_loop(0, rows // 8, cells, 0)

    own_high = HIGH // owners
    together = 4

    def offsets(step, carry):
        first = step * together
        totals = [jnp.zeros((HIGH, LANES), f32)] * together
        squares = [jnp.zeros((HIGH, LANES), f32)] * together
        for c in range(rows):
            off = compact_ref[pl.ds(c * 2 * HIGH, HIGH), :]
            value = compact_ref[pl.ds(c * 2 * HIGH + HIGH, HIGH), :]
            for u in range(together):
                mine = jnp.where(off == (first + u).astype(f32), value, f32(0.0))
                totals[u] = totals[u] + mine
                squares[u] = squares[u] + mine * mine
        for u in range(together):
            total_s[0] = totals[u]
            total_s[1] = squares[u]
            for d in range(owners):
                start = lax.rem(owner_ref[0] + d, owners) * own_high
                for s in range(2):
                    target = ((first + u) * 2 + s) * own_high
                    total_refs[d][pl.ds(target, own_high), :] = total_s[s, pl.ds(start, own_high), :]
        return carry

    lax.fori_loop(0, STRIDE // together, offsets, 0)


def select_kernel(owner_ref, compact_ref, scale_ref, selected_ref, *refs, owners):
    dense_refs = refs[:owners]
    sum_refs = refs[owners:2 * owners]
    pairs_s = refs[2 * owners]
    rows = scale_ref.shape[0]
    share = selected_ref.shape[1] // owners
    share_rows = share // LANES
    width = min(256, share)
    for h in range(HIGH):
        lanes = pl.ds((h % 2) * LANES, LANES)
        pairs_s[h // 2, pl.ds(0, rows), lanes] = compact_ref[
            pl.ds(h, rows, stride=2 * HIGH), :
        ].astype(bf16)
        value = compact_ref[pl.ds(HIGH + h, rows, stride=2 * HIGH), :]
        upper = value.astype(bf16)
        pairs_s[h // 2, pl.ds(rows, rows), lanes] = upper
        pairs_s[h // 2, pl.ds(2 * rows, rows), lanes] = (value - upper.astype(f32)).astype(bf16)
    ids = lax.broadcasted_iota(jnp.int32, (16, width), 0).astype(f32).astype(bf16)
    for d in range(owners):
        owner = lax.rem(owner_ref[0] + d, owners)
        for start in range(0, share, width):
            place = pl.multiple_of(owner * share + start, LANES)
            picked = selected_ref[:, pl.ds(place, width)]
            low16 = jnp.broadcast_to(
                ((picked >> STRIDE_BITS) & (LANES - 1)).astype(f32), (16, width)
            ).astype(bf16)
            high16 = jnp.broadcast_to(
                (picked >> ROW_BITS).astype(f32), (16, width)
            ).astype(bf16)
            low_hot = one_hot_lanes(low16, ids, LANES)
            acc = jnp.zeros((3 * rows, width), f32)
            for pair in range(HIGH // 2):
                parts = []
                for h in (2 * pair, 2 * pair + 1):
                    hit = high16 == bf16(float(h))
                    parts += [jnp.where(hit, part, bf16(0.0)) for part in low_hot]
                acc = acc + jnp.dot(
                    pairs_s[pair], jnp.concatenate(parts, axis=0), preferred_element_type=f32
                )
            off = (picked & (STRIDE - 1)).astype(f32)
            value = acc[rows:2 * rows] + acc[2 * rows:]
            dense = jnp.where(acc[:rows] == off, value, f32(0.0))
            dense_refs[d][:, pl.ds(start, width)] = dense.astype(dense_refs[d].dtype)
            stats = [
                jnp.sum(dense, axis=0, keepdims=True),
                jnp.sum(dense * dense, axis=0, keepdims=True),
            ]
            for s in range(2):
                for q in range(width // LANES):
                    target = s * share_rows + start // LANES + q
                    sum_refs[d][pl.ds(target, 1), :] = stats[s][:, q * LANES:(q + 1) * LANES]


def shift(value, axis, d):
    n = lax.axis_size(axis)
    return lax.ppermute(value, axis, [(s, (s + d) % n) for s in range(n)])


def paired(n):
    return n & (n - 1) == 0


def exchange(value, axis, d):
    n = lax.axis_size(axis)
    if not paired(n):
        return shift(value, axis, d)
    return lax.ppermute(value, axis, [(s, s ^ d) for s in range(n)])


def tree_sum(terms):
    while len(terms) > 1:
        last = terms[len(terms) - len(terms) % 2:]
        terms = [terms[i] + terms[i + 1] for i in range(0, len(terms) - 1, 2)] + last
    return terms[0]


def target_of(place, d, n):
    return place ^ d if paired(n) else lax.rem(place + d, n)


def slot_of(place, i, n):
    return place ^ i if paired(n) else lax.rem(place + n - i, n)


def per_device(columns, counts, nnz_count, selected):
    rows, slots = columns.shape
    sel = selected.shape[0]
    owners = lax.axis_size("gz")
    outer = lax.axis_size("gx")
    middle = lax.axis_size("gy")
    cells = rows * outer * middle * owners
    owner = lax.axis_index("gz")
    place = lax.axis_index("gx")
    share = sel // owners
    own_high = HIGH // owners
    sum_rows = STRIDE * 2 * own_high
    vmem = pl.BlockSpec(memory_space=pltpu.VMEM)
    smem = pl.BlockSpec(memory_space=pltpu.SMEM)
    owner_arg = owner.reshape(1).astype(jnp.int32)

    made = pl.pallas_call(
        functools.partial(scatter_kernel, owners=owners),
        out_shape=[
            jax.ShapeDtypeStruct((rows * 2 * HIGH, LANES), f32),
            jax.ShapeDtypeStruct((rows, LANES), f32),
        ] + [jax.ShapeDtypeStruct((sum_rows, LANES), f32)] * owners,
        in_specs=[smem, vmem, vmem, vmem],
        out_specs=[vmem] * (2 + owners),
        scratch_shapes=[pltpu.VMEM((rows, slots), f32)] * 4 + [pltpu.VMEM((2, HIGH, LANES), f32)],
        name="scatter",
    )(owner_arg, columns, counts, nnz_count.reshape(1, rows))
    compact, scale, sums = made[0], made[1], made[2:]
    moved_sums = [shift(sums[d], "gz", d) for d in range(1, owners)]

    picked = pl.pallas_call(
        functools.partial(select_kernel, owners=owners),
        out_shape=[jax.ShapeDtypeStruct((rows, share), f32)]
        + [jax.ShapeDtypeStruct((rows, share), bf16)] * (owners - 1)
        + [jax.ShapeDtypeStruct((2 * share // LANES, LANES), f32)] * owners,
        in_specs=[smem, vmem, vmem, vmem],
        out_specs=[vmem] * (2 * owners),
        scratch_shapes=[pltpu.VMEM((HIGH // 2, 3 * rows, 2 * LANES), bf16)],
        name="select",
    )(owner_arg, compact, scale, selected.reshape(1, sel))
    own_sums, *picked = lax.optimization_barrier((sums[0], *picked))
    dense, picked_sums = picked[:owners], picked[owners:]
    moved_picked = [shift(picked_sums[d], "gz", d) for d in range(1, owners)]
    moved_dense = [shift(dense[d], "gz", d) for d in range(1, owners)]

    gene_sums = functools.reduce(jnp.add, [own_sums] + moved_sums)
    sel_sums = functools.reduce(jnp.add, [picked_sums[0]] + moved_picked)
    chunk_rows = sum_rows // outer
    chunks = gene_sums.reshape(outer, chunk_rows, LANES)

    def chunk(d):
        return lax.dynamic_index_in_dim(chunks, target_of(place, d, outer), 0, keepdims=False)

    part = functools.reduce(
        jnp.add, [chunk(0)] + [exchange(chunk(d), "gx", d) for d in range(1, outer)]
    )
    part = jnp.concatenate([part, sel_sums], axis=0)
    part = tree_sum([part] + [exchange(part, "gy", d) for d in range(1, middle)])
    held = jnp.stack([part] + [exchange(part, "gx", d) for d in range(1, outer)])
    full = jnp.stack(
        [
            lax.dynamic_index_in_dim(held[:, :chunk_rows], slot_of(place, i, outer), 0, keepdims=False)
            for i in range(outer)
        ]
    )
    genes = full.reshape(STRIDE, 2, own_high * LANES)
    mean = genes[:, 0] / cells
    variance = genes[:, 1] / cells - mean * mean
    gene_stats = jnp.stack([mean, variance]).transpose(0, 2, 1).reshape(2, -1)
    sel_full = jnp.sum(held[:, chunk_rows:], axis=0).reshape(2, share)
    sel_mean = sel_full[0] / cells
    sel_variance = sel_full[1] / cells - sel_mean * sel_mean
    sel_scale = jnp.sqrt(jnp.maximum(sel_variance, var_floor))
    blocks = jnp.stack([dense[0]] + [m.astype(f32) for m in moved_dense])
    ordered = jnp.concatenate(
        [
            lax.dynamic_index_in_dim(blocks, lax.rem(owner + owners - q, owners), 0, keepdims=False)
            for q in range(owners)
        ],
        axis=0,
    )
    pca_input = jnp.clip((ordered - sel_mean) / sel_scale, -clip_value, clip_value).astype(bf16)
    return (gene_stats, pca_input)


def solution(mesh):
    return jax.shard_map(
        per_device,
        mesh=mesh,
        in_specs=(
            P(("gx", "gy", "gz"), None),
            P(("gx", "gy", "gz"), None),
            P(("gx", "gy", "gz")),
            P(),
        ),
        out_specs=(P(None, "gz"), P(("gx", "gy"), "gz")),
        check_vma=False,
    )
```
